32 devices in a mesh: grp: 4 (over z), cand: 8 (over y, x, core).
Axes of the slice: x: 2, y: 2, z: 4, core: 2. Of those that a mesh axis runs over, the one named last changes fastest.
Arguments:
- embeddings: bfloat16 [96, 1024, 1024], P('grp', 'cand'), may hold values from -6 to 6
- hidden_weight: bfloat16 [2048, 1024], P('cand'), may hold values from -0.1875 to 0.1875
- score_weight: bfloat16 [2048], replicated, may hold values from -0.5 to 0.5
- relevance: int32 [96, 1024], P('grp', 'cand'), may hold values from 0 to 4
- rank_pos: int32 [96, 1024], P('grp', 'cand'), may hold values from 0 to 1023, as said below
- ideal_dcg: float32 [96], P('grp'), may hold values from 32 to 128
Outputs:
- grad_hidden: float32 [2048, 1024], P('cand')
- lambdas: float32 [96, 1024], P('grp', 'cand')
The draws below stay inside these ranges and needn't reach their ends.
Inputs may be any that keep to these rules, and one draw needn't show every extreme that they name: `rank_pos`: in each group the rank positions are a permutation of 0 to 1023.
All inputs are finite; a program needn't handle non-finite values.
Results may differ from the reference program's by a relative error of at most 0.006.
Values may be sent and summed in bfloat16 or wider, within the bound.
A program may use at most 64 MiB of HBM per device.

```python
import math
import jax
import jax.numpy as jnp
from jax import lax

EMBED = 1024
HIDDEN_SIZE = 2048
CANDS = 1024
GRP_DEV = 24
GROUPS = 96
N_GRP = 4
N_CAND = 8


def draw_rank_pos(key, part):
    jitter = jax.random.randint(jax.random.fold_in(key, 11), (GROUPS, CANDS), 0, CANDS // 4)
    order_key = jnp.arange(CANDS, dtype=jnp.int32)[None, :] * 4 + jitter
    order = jnp.argsort(order_key, axis=1, stable=True)
    return jnp.argsort(order, axis=1, stable=True).astype(jnp.int32)


def place_ends(array, rng, smallest, high):
    longest = array.shape.index(max(array.shape))
    spots = []
    for shift in (0, 1):
        where = [jax.random.randint(jax.random.fold_in(rng, axis), (), 0, length) for axis, length in enumerate(array.shape)]
        where[longest] = (where[longest] + shift) % array.shape[longest]
        spots.append(tuple(where))
    return array.at[spots[0]].set(smallest).at[spots[1]].set(high)


def block_scale(rng, dims, cuts, least, top_value):
    def one(axis_at, blocks):
        steps = jax.random.uniform(jax.random.fold_in(jax.random.fold_in(rng, 6), axis_at), (blocks,), jnp.float32, least / len(cuts), top_value / len(cuts))
        return jnp.repeat(jnp.exp(steps), dims[axis_at] // blocks).reshape((-1,) + (1,) * (len(dims) - axis_at - 1))

    gain = one(*cuts[0])
    for cut in cuts[1:]:
        gain = gain * one(*cut)
    return gain


def normal_values(key, dims, spread, most, shards=(), held_as=jnp.bfloat16):
    array = spread * jax.random.normal(key, dims, jnp.float32)
    if shards:
        array = array * block_scale(key, dims, shards, -0.22, 0.18)
    return jnp.clip(array, -most, most).astype(held_as)


def setup_inputs(seed: int = 0) -> dict:
    key_of = jax.random.split(jax.random.key(seed), 7)
    embeddings = normal_values(key_of[0], (GROUPS, CANDS, EMBED), 1.0, 6.0, ((0, 4), (1, 8)))
    hidden_weight = normal_values(key_of[1], (HIDDEN_SIZE, EMBED), EMBED ** -0.5, 0.1875, ((0, 8),))
    score_weight = normal_values(key_of[2], (HIDDEN_SIZE,), (HIDDEN_SIZE // 16) ** -0.5, 0.5)
    relevance = place_ends(jax.random.randint(key_of[3], (GROUPS, CANDS), 0, 5), jax.random.fold_in(key_of[3], 1), 0, 4).astype(jnp.int32)
    rank_pos = draw_rank_pos(jax.random.fold_in(key_of[6], 71), 0)
    ideal_dcg = jnp.clip(jnp.exp(math.log(128.0) - 1.3862944 * jax.random.uniform(key_of[5], (GROUPS,), jnp.float32) ** block_scale(key_of[5], (GROUPS,), ((0, 4),), -0.2, 0.2)), 32.0, 128.0)
    return dict(embeddings=embeddings, hidden_weight=hidden_weight, score_weight=score_weight, relevance=relevance, rank_pos=rank_pos, ideal_dcg=ideal_dcg)


EPS = 1e-06

def pair_lambdas(own_score, own_gain, own_disc, far_score, far_gain, far_disc, ideal):
    gain_diff = far_gain[..., None, :] - own_gain[..., :, None]
    toward = jnp.sign(gain_diff)
    weight = jnp.abs(gain_diff) * jnp.abs(far_disc[..., None, :] - own_disc[..., :, None]) / ideal[..., None, None]
    margin = own_score[..., :, None] - far_score[..., None, :]
    return lax.optimization_barrier(jnp.sum(weight * toward * jax.nn.sigmoid(toward * margin), axis=-1))

def reference(embeddings, hidden_weight, score_weight, relevance, rank_pos, ideal_dcg):

    def group_scores(cand_rows):
        pre_act = jnp.dot(cand_rows, hidden_weight.T, preferred_element_type=jnp.float32)
        acts = jax.nn.gelu(pre_act).astype(jnp.bfloat16)
        return jnp.dot(acts, score_weight, preferred_element_type=jnp.float32)
    scores = lax.map(group_scores, embeddings)
    gain_vals = jnp.exp2(relevance.astype(jnp.float32)) - 1.0
    discount = 1.0 / jnp.log2(2.0 + rank_pos.astype(jnp.float32))

    def group_lambdas(packed):
        own_score, own_gain, own_disc, ideal = packed
        return pair_lambdas(own_score, own_gain, own_disc, own_score, own_gain, own_disc, ideal)
    lambdas = lax.map(group_lambdas, (scores, gain_vals, discount, ideal_dcg))
    local = CANDS // N_CAND
    weight_row = score_weight.astype(jnp.float32)
    zero_index = jnp.zeros((), jnp.int32)

    def add_block(running, index):
        first = (index // N_CAND * GRP_DEV).astype(jnp.int32)
        cand_first = (index % N_CAND * local).astype(jnp.int32)
        block = lax.dynamic_slice(embeddings, (first, cand_first, zero_index), (GRP_DEV, local, EMBED))
        cand_rows = block.reshape(GRP_DEV * local, EMBED)
        block_lam = lax.dynamic_slice(lambdas, (first, cand_first), (GRP_DEV, local)).reshape(GRP_DEV * local)
        pre_act = jnp.dot(cand_rows, hidden_weight.T, preferred_element_type=jnp.float32)
        _, pull = jax.vjp(jax.nn.gelu, pre_act)
        upstream = block_lam[:, None] * weight_row[None, :]
        grad_pre = pull(upstream)[0].astype(jnp.bfloat16)
        term = lax.dot_general(grad_pre, cand_rows, (((0,), (0,)), ((), ())), preferred_element_type=jnp.float32)
        rounded = lax.optimization_barrier(term.astype(jnp.bfloat16))
        return (running + rounded.astype(jnp.float32), None)
    total, _ = lax.scan(add_block, jnp.zeros((HIDDEN_SIZE, EMBED), jnp.float32), jnp.arange(N_GRP * N_CAND, dtype=jnp.int32))
    scale = lax.rsqrt(jnp.mean(total * total) + EPS)
    return (total * scale, lambdas)
```

```python
import functools

import jax
import jax.numpy as jnp
from jax import lax
from jax.experimental import pallas as pl
from jax.experimental.pallas import tpu as pltpu
from jax.sharding import PartitionSpec as P

EPS = 1e-06


def pair_lambdas(own_score, own_gain, own_disc, far_score, far_gain, far_disc, ideal):
    gain_diff = far_gain[..., None, :] - own_gain[..., :, None]
    toward = jnp.sign(gain_diff)
    weight = (
        jnp.abs(gain_diff)
        * jnp.abs(far_disc[..., None, :] - own_disc[..., :, None])
        / ideal[..., None, None]
    )
    margin = own_score[..., :, None] - far_score[..., None, :]
    return jnp.sum(weight * toward * jax.nn.sigmoid(toward * margin), axis=-1)


def gain_of(labels):
    return jnp.exp2(labels.astype(jnp.float32)) - 1.0


def discount_of(positions):
    return 1.0 / jnp.log2(2.0 + positions.astype(jnp.float32))


def per_device_plain(embeddings, hidden_weight, score_weight, relevance, rank_pos, ideal_dcg):
    grp_count, local, width = embeddings.shape
    cand_rows = embeddings.reshape(grp_count * local, width)
    pre_act = lax.dot_general(
        cand_rows,
        lax.all_gather(hidden_weight, "cand", axis=0, tiled=True),
        (((1,), (1,)), ((), ())),
        preferred_element_type=jnp.float32,
    )
    acts, pull = jax.vjp(jax.nn.gelu, pre_act)
    scores = jnp.dot(
        acts.astype(jnp.bfloat16), score_weight, preferred_element_type=jnp.float32
    ).reshape(grp_count, local)
    gain_vals = gain_of(relevance)
    discount = discount_of(rank_pos)
    lambdas = pair_lambdas(
        scores,
        gain_vals,
        discount,
        lax.all_gather(scores, "cand", axis=1, tiled=True),
        lax.all_gather(gain_vals, "cand", axis=1, tiled=True),
        lax.all_gather(discount, "cand", axis=1, tiled=True),
        ideal_dcg,
    )
    upstream = (
        lambdas.reshape(grp_count * local)[:, None] * score_weight.astype(jnp.float32)[None, :]
    )
    grad_pre = pull(upstream)[0].astype(jnp.bfloat16)
    owned = lax.psum_scatter(
        lax.dot_general(
            grad_pre, cand_rows, (((0,), (0,)), ((), ())), preferred_element_type=jnp.float32
        ).astype(jnp.bfloat16),
        "cand",
        scatter_dimension=0,
        tiled=True,
    ).astype(jnp.float32)
    summed = lax.psum(owned, "grp")
    squares = lax.psum(jnp.sum(summed * summed), "cand")
    entries = summed.shape[0] * summed.shape[1] * lax.axis_size("cand")
    scale = lax.rsqrt(squares / entries + EPS)
    return (summed * scale, lambdas)


MESH = pl.DeviceIdType.MESH
GELU_C = 0.7978845608028654
GELU_A = 0.044715
PLANE = 8
LANES = 128
W_DIRECT = [(0, 0, 1), (0, 1, 1), (0, 0, 4), (0, 1, 2), (0, 0, 2), (0, 1, 4)]


def step_kernel(
    groups,
    emb_hbm,
    w_hbm,
    sw_ref,
    gd_ref,
    hinv_ref,
    tot_ref,
    sq_ref,
    lam_ref,
    emb,
    wall,
    dpre,
    gbuf,
    scacc,
    all_s,
    all_gd,
    cols,
    lam_t,
    lrow,
    p_send,
    p_recv,
    s6,
    s2,
    s4,
    t32,
    x4,
    y2,
    x0,
    y0,
    zs,
    zr,
    sq_all,
    loc_sem,
    w_ss,
    w_rs,
    g_ss,
    g_rs,
    s_ss,
    s_rs,
    p_ss,
    p_rs,
    a_ss,
    a_rs,
    z_ss,
    z_rs,
    q_ss,
    q_rs,
):
    c = lax.axis_index("cand")
    z = lax.axis_index("grp")
    n_z = zr.shape[0] + 1
    hs = wall.shape[1]
    half = hs // 2
    rows, width = emb.shape

    def flip(value, mask):
        out, bit = 0, 1
        while bit < PLANE:
            b = (value // bit) % 2
            out = out + bit * ((1 - b) if mask & bit else b)
            bit *= 2
        return out

    def zflip(mask):
        out, bit = 0, 1
        while bit < n_z:
            b = (z // bit) % 2
            out = out + bit * ((1 - b) if mask & bit else b)
            bit *= 2
        return out

    def to(r):
        return {"cand": flip(c, r)}

    def tz(q):
        return {"grp": zflip(q)}

    def remote(src, dst, ss, rs, dev):
        return pltpu.make_async_remote_copy(
            src_ref=src, dst_ref=dst, send_sem=ss, recv_sem=rs, device_id=dev, device_id_type=MESH
        )

    w_in = pltpu.make_async_copy(w_hbm, wall.at[0], loc_sem.at[0])
    e_in = pltpu.make_async_copy(emb_hbm, emb, loc_sem.at[1])
    g_in = pltpu.make_async_copy(gd_ref, all_gd.at[0], loc_sem.at[2])
    w_in.start()
    g_in.start()
    e_in.start()

    barrier = pltpu.get_barrier_semaphore()
    for r in range(1, PLANE):
        pl.semaphore_signal(barrier, inc=1, device_id=to(r), device_id_type=MESH)
    for q in range(1, n_z):
        pl.semaphore_signal(barrier, inc=1, device_id=tz(q), device_id_type=MESH)
    pl.semaphore_wait(barrier, PLANE - 1 + n_z - 1)

    def w_copy(src, h, hop):
        dst = src ^ hop
        part = pl.ds(h * half, half)
        return remote(
            wall.at[src, part], wall.at[dst, part], w_ss.at[dst, h], w_rs.at[dst, h], to(hop)
        )

    started = []

    def go(copy):
        copy.start()
        started.append(copy)
        return copy

    w_in.wait()
    by_dst = {}
    for src, h, hop in W_DIRECT:
        by_dst[src ^ hop, h] = go(w_copy(src, h, hop))
    g_in.wait()
    gd_copies = [
        go(remote(all_gd.at[0], all_gd.at[r], g_ss.at[r - 1], g_rs.at[r - 1], to(r)))
        for r in range(1, PLANE)
    ]
    e_in.wait()

    scacc[...] = jnp.zeros_like(scacc)
    tile = 2 * LANES
    inner = 3 if rows % (3 * tile) == 0 else 1

    def forward_block(r):
        blk = pl.multiple_of(flip(c, r) * hs, hs)
        sw = sw_ref[pl.ds(blk, hs), :]

        @pl.loop(0, rows // (tile * inner))
        def _(step):
            for u in range(inner):
                at = pl.multiple_of((step * inner + u) * tile, tile)
                x = lax.dot_general(
                    wall[r],
                    emb[pl.ds(at, tile), :],
                    (((1,), (1,)), ((), ())),
                    preferred_element_type=jnp.float32,
                )
                x2 = x * x
                t = jnp.tanh(x * (GELU_C + (GELU_C * GELU_A) * x2))
                h = 0.5 + 0.5 * t
                act = x * h
                slope = h + act * ((1.0 - h) * (2 * GELU_C + (6 * GELU_C * GELU_A) * x2))
                dpre[r, :, pl.ds(at, tile)] = slope * sw
                scacc[:, pl.ds(at, tile)] += jnp.sum(
                    (act * sw).reshape(hs // 8, 8, tile), axis=0
                )

    def arrived(r, h):
        by_dst[r, h].wait_recv()

    def pass_on(src, h, hop):
        by_dst[src ^ hop, h] = go(w_copy(src, h, hop))

    forward_block(0)
    arrived(1, 0)
    arrived(1, 1)
    forward_block(1)
    arrived(4, 0)
    pass_on(4, 0, 2)
    pass_on(4, 0, 1)
    arrived(2, 1)
    pass_on(2, 1, 4)
    pass_on(2, 1, 1)
    arrived(2, 0)
    pass_on(2, 0, 1)
    arrived(4, 1)
    pass_on(4, 1, 1)
    forward_block(2)
    forward_block(4)
    arrived(3, 0)
    arrived(3, 1)
    forward_block(3)
    arrived(6, 0)
    pass_on(6, 0, 1)
    arrived(6, 1)
    pass_on(6, 1, 1)
    arrived(5, 0)
    arrived(5, 1)
    forward_block(5)
    forward_block(6)
    arrived(7, 0)
    arrived(7, 1)
    forward_block(7)

    score_row = 0.5 * jnp.sum(scacc[...], axis=0, keepdims=True)
    for g in range(groups):
        all_s[0, g : g + 1, :] = score_row[:, g * LANES : (g + 1) * LANES]
    s_copies = [
        go(remote(all_s.at[0], all_s.at[r], s_ss.at[r - 1], s_rs.at[r - 1], to(r)))
        for r in range(1, PLANE)
    ]

    fill = jnp.zeros((LANES - groups, LANES), jnp.float32)

    def turned(value):
        return jnp.transpose(jnp.concatenate([value, fill], axis=0))

    cols[0] = turned(all_s[0])
    cols[1] = turned(all_gd[0, 0])
    cols[2] = turned(all_gd[0, 1])
    for copy in gd_copies:
        copy.wait_recv()
    for copy in s_copies:
        copy.wait_recv()

    lam_t[...] = jnp.zeros_like(lam_t)
    for g in range(groups):
        si = jnp.broadcast_to(cols[0, :, g : g + 1], (LANES, LANES))
        gi = jnp.broadcast_to(cols[1, :, g : g + 1], (LANES, LANES))
        di = jnp.broadcast_to(cols[2, :, g : g + 1], (LANES, LANES))
        acc = jnp.zeros((LANES, LANES), jnp.float32)
        for r in range(PLANE):
            gain_diff = all_gd[r, 0, g : g + 1, :] - gi
            far = jnp.abs(all_gd[r, 1, g : g + 1, :] - di)
            t = jnp.tanh(si - all_s[r, g : g + 1, :])
            acc = acc + far * (gain_diff + jnp.abs(gain_diff) * t)
        lam_t[:, g : g + 1] = jnp.sum(acc, axis=1, keepdims=True)
    lam = jnp.transpose(lam_t[...])[:groups, :] * hinv_ref[...]
    lam_ref[...] = lam
    for g in range(groups):
        lrow[:, g * LANES : (g + 1) * LANES] = lam[g : g + 1, :]

    ntile = 2 * LANES

    def grad_block(r, finish):
        @pl.loop(0, rows // (2 * tile))
        def _(step):
            at = pl.multiple_of(step * 2 * tile, 2 * tile)
            part = pl.ds(at, 2 * tile)
            gbuf[:, part] = (dpre[r, :, part] * lrow[:, part]).astype(jnp.bfloat16)

        @pl.loop(0, width // ntile)
        def _(step):
            at = pl.multiple_of(step * ntile, ntile)
            part = pl.ds(at, ntile)
            finish(
                part,
                jnp.dot(gbuf[...], emb[:, part], preferred_element_type=jnp.float32),
            )

    def odd(r):
        slot = r // 2

        def finish(part, value):
            p_send[slot, :, part] = value.astype(jnp.bfloat16)

        grad_block(r, finish)
        return go(remote(p_send.at[slot], p_recv.at[slot], p_ss.at[slot], p_rs.at[slot], to(1)))

    def even(r, copy, out):
        def finish(part, value):
            out[:, part] = value.astype(out.dtype)

        grad_block(r, finish)
        copy.wait_recv()

    def chip_sum(r, copy, out):
        even(r, copy, t32)
        out_value = t32[...] + p_recv[r // 2].astype(jnp.float32)
        if out is None:
            t32[...] = out_value
        else:
            out[...] = out_value.astype(out.dtype)

    low, high = pl.ds(0, half), pl.ds(half, half)

    def axis_copy(i, src, dst, hop):
        return go(remote(src, dst, a_ss.at[i], a_rs.at[i], to(hop)))

    copy = odd(7)
    chip_sum(6, copy, s6)
    to_x4 = axis_copy(0, s6.at[low], x4, 2)
    to_y2 = axis_copy(1, s6.at[high], y2, 4)
    copy = odd(3)
    chip_sum(2, copy, None)
    s2[low, :] = t32[low, :].astype(jnp.bfloat16)
    x0_low = axis_copy(2, s2.at[low], x0.at[low], 2)
    zs[...] = t32[...]
    copy = odd(5)
    to_y2.wait_recv()
    s2[high, :] = (zs[high, :] + y2[...].astype(jnp.float32)).astype(jnp.bfloat16)
    x0_high = axis_copy(3, s2.at[high], x0.at[high], 2)
    chip_sum(4, copy, None)
    s4[high, :] = t32[high, :].astype(jnp.bfloat16)
    y0_high = axis_copy(4, s4.at[high], y0.at[high], 4)
    to_x4.wait_recv()
    s4[low, :] = (t32[low, :] + x4[...].astype(jnp.float32)).astype(jnp.bfloat16)
    y0_low = axis_copy(5, s4.at[low], y0.at[low], 4)
    copy = odd(1)
    chip_sum(0, copy, None)
    for copy in (x0_low, y0_high, x0_high, y0_low):
        copy.wait_recv()
    t32[...] = t32[...] + x0[...].astype(jnp.float32) + y0[...].astype(jnp.float32)

    zpart = hs // n_z
    s6_done, s6_done2 = to_x4, to_y2
    s6_done.wait_send()
    s6_done2.wait_send()
    s6[...] = t32[...].astype(jnp.bfloat16)

    def zrows(index):
        return pl.ds(pl.multiple_of(index * zpart, zpart), zpart)

    z_copies = [
        go(remote(s6.at[zrows(zflip(q))], zr.at[q - 1], z_ss.at[q - 1], z_rs.at[q - 1], tz(q)))
        for q in range(1, n_z)
    ]
    part = t32[zrows(z), :]
    for q, copy in enumerate(z_copies):
        copy.wait_recv()
        part = part + zr[q].astype(jnp.float32)
    tot_ref[zrows(z), :] = part.astype(jnp.bfloat16)
    out_copies = [
        go(
            remote(
                tot_ref.at[zrows(z)],
                tot_ref.at[zrows(z)],
                z_ss.at[n_z - 2 + q],
                z_rs.at[n_z - 2 + q],
                tz(q),
            )
        )
        for q in range(1, n_z)
    ]
    for copy in out_copies:
        copy.wait_recv()
    total = tot_ref[...].astype(jnp.float32)
    sq_all[0] = jnp.sum((total * total).reshape(hs // 8, 8, width), axis=0).reshape(
        8, width // LANES, LANES
    ).sum(axis=1)
    q_copies = [
        go(remote(sq_all.at[0], sq_all.at[r], q_ss.at[r - 1], q_rs.at[r - 1], to(r)))
        for r in range(1, PLANE)
    ]
    for copy in q_copies:
        copy.wait_recv()
    sq_ref[...] = jnp.sum(sq_all[...], axis=0)
    done = (to_x4, to_y2)
    for copy in started:
        if copy is not done[0] and copy is not done[1]:
            copy.wait_send()


def per_device_fused(embeddings, hidden_weight, score_weight, relevance, rank_pos, ideal_dcg):
    groups, local, width = embeddings.shape
    rows = groups * local
    hs = hidden_weight.shape[0]
    hidden = score_weight.shape[0]
    n_z = lax.axis_size("grp")
    gain_disc = jnp.stack([gain_of(relevance), discount_of(rank_pos)])
    hinv = jnp.broadcast_to((0.5 / ideal_dcg)[:, None], (groups, local))
    bf, f32 = jnp.bfloat16, jnp.float32
    vmem = pl.BlockSpec(memory_space=pltpu.VMEM)
    hbm = pl.BlockSpec(memory_space=pl.ANY)
    dma = pltpu.SemaphoreType.DMA
    half = hs // 2
    total, squares, lambdas = pl.pallas_call(
        functools.partial(step_kernel, groups),
        out_shape=(
            jax.ShapeDtypeStruct((hs, width), bf),
            jax.ShapeDtypeStruct((8, LANES), f32),
            jax.ShapeDtypeStruct((groups, local), f32),
        ),
        in_specs=[hbm, hbm, vmem, hbm, vmem],
        out_specs=(vmem, vmem, vmem),
        scratch_shapes=[
            pltpu.VMEM((rows, width), bf),
            pltpu.VMEM((PLANE, hs, width), bf),
            pltpu.VMEM((PLANE, hs, rows), f32),
            pltpu.VMEM((hs, rows), bf),
            pltpu.VMEM((8, rows), f32),
            pltpu.VMEM((PLANE, groups, local), f32),
            pltpu.VMEM((PLANE, 2, groups, local), f32),
            pltpu.VMEM((3, LANES, LANES), f32),
            pltpu.VMEM((LANES, LANES), f32),
            pltpu.VMEM((1, rows), f32),
            pltpu.VMEM((PLANE // 2, hs, width), bf),
            pltpu.VMEM((PLANE // 2, hs, width), bf),
            pltpu.VMEM((hs, width), bf),
            pltpu.VMEM((hs, width), bf),
            pltpu.VMEM((hs, width), bf),
            pltpu.VMEM((hs, width), f32),
            pltpu.VMEM((half, width), bf),
            pltpu.VMEM((half, width), bf),
            pltpu.VMEM((hs, width), bf),
            pltpu.VMEM((hs, width), bf),
            pltpu.VMEM((hs, width), f32),
            pltpu.VMEM((n_z - 1, hs // n_z, width), bf),
            pltpu.VMEM((PLANE, 8, LANES), f32),
            dma((3,)),
            dma((PLANE, 2)),
            dma((PLANE, 2)),
            dma((PLANE - 1,)),
            dma((PLANE - 1,)),
            dma((PLANE - 1,)),
            dma((PLANE - 1,)),
            dma((PLANE // 2,)),
            dma((PLANE // 2,)),
            dma((6,)),
            dma((6,)),
            dma((2 * (n_z - 1),)),
            dma((2 * (n_z - 1),)),
            dma((PLANE - 1,)),
            dma((PLANE - 1,)),
        ],
        compiler_params=pltpu.CompilerParams(
            collective_id=0, has_side_effects=True, vmem_limit_bytes=64000 * 1024
        ),
    )(
        embeddings.reshape(rows, width),
        hidden_weight,
        score_weight.astype(f32).reshape(hidden, 1),
        gain_disc,
        hinv,
    )
    scale = lax.rsqrt(jnp.sum(squares) / (hidden * width) + EPS)
    return (total.astype(f32) * scale, lambdas)


def choose(embeddings, hidden_weight, *rest):
    groups, local, width = embeddings.shape
    n_z = lax.axis_size("grp")
    fits = (
        lax.axis_size("cand") == PLANE
        and local == LANES
        and groups <= LANES
        and (groups * local) % (4 * LANES) == 0
        and width % (2 * LANES) == 0
        and n_z > 1
        and n_z & (n_z - 1) == 0
        and hidden_weight.shape[0] % (16 * n_z) == 0
    )
    body = per_device_fused if fits else per_device_plain
    return body(embeddings, hidden_weight, *rest)


def solution(mesh):
    return jax.shard_map(
        choose,
        mesh=mesh,
        in_specs=(
            P("grp", "cand", None),
            P("cand", None),
            P(),
            P("grp", "cand"),
            P("grp", "cand"),
            P("grp"),
        ),
        out_specs=(P("cand", None), P("grp", "cand")),
        check_vma=False,
    )
```
